128 devices in a mesh: gz: 4 (over x), row: 8 (over z, core), col: 4 (over y).
Axes of the slice: x: 4, y: 4, z: 4, core: 2. Of those that a mesh axis runs over, the one named last changes fastest.
Arguments:
- leaf_probe: bfloat16 [128, 512, 128], P(('gz', 'row', 'col')), may hold values from -6 to 6
- leaf_lower_inv: bfloat16 [128, 512, 512], P(('gz', 'row', 'col')), may hold values from -0.25 to 0.25
- leaf_upper_inv: bfloat16 [128, 512, 512], P(('gz', 'row', 'col')), may hold values from -0.25 to 0.25
- leaf_lower_panel: bfloat16 [128, 1024, 512], P(('gz', 'row', 'col')), may hold values from -0.09375 to 0.09375
- leaf_upper_panel: bfloat16 [128, 512, 1024], P(('gz', 'row', 'col')), may hold values from -0.1875 to 0.1875
- leaf_tiles: int32 [128], P(('gz', 'row', 'col')), may hold values from 1 to 4, as said below
- coupled: int32 [128, 8], P(('gz', 'row', 'col')), may hold values from 0 to 127, as said below
- top_probe: bfloat16 [4, 4096, 128], P(None, ('row', 'col')), may hold values from -6 to 6
- top_lower_inv: bfloat16 [4, 4096, 4096], P(None, ('row', 'col')), may hold values from -0.09375 to 0.09375
- top_lower_blocks: bfloat16 [6, 4096, 4096], P(None, ('row', 'col')), may hold values from -0.0625 to 0.0625
- top_upper_inv: bfloat16 [4, 4096, 4096], P(None, ('row', 'col')), may hold values from -0.09375 to 0.09375
- top_upper_blocks: bfloat16 [6, 4096, 4096], P(None, ('row', 'col')), may hold values from -0.0625 to 0.0625
Outputs:
- leaf_solution: float32 [128, 512, 128], P(('gz', 'row', 'col'))
- top_solution: float32 [4, 4096, 128], P(None, ('row', 'col'))
The draws below stay inside these ranges and needn't reach their ends.
Inputs may be any that keep to these rules, and one draw needn't show every extreme that they name: `leaf_tiles`: some leaf has 4 blocks. `coupled`: the 8 numbers of one leaf are distinct.
All inputs are finite; a program needn't handle non-finite values.
Results may differ from the reference program's by a relative error of at most 0.02.
Values may be sent and summed in bfloat16 or wider, within the bound.
No kernel may reach another device: no remote copies, remote signals or barrier semaphores. Data moves between devices by JAX's collectives and lax.ppermute only.
A program may use at most 128 MiB of HBM per device.

```python
import jax
import jax.numpy as jnp
from jax import lax

COLS = 128
TILE = 128
WL = 512
NCT = 8
LEVELS = 4
PAIRS = 6
LEAVES = 128
SEP = 4096
ANC_TILES = 128


def draw_leaf_tiles(key, part):
    first_key, second_key = jax.random.split(jax.random.fold_in(key, 11))
    drawn = jax.random.randint(first_key, (LEAVES,), 1, WL // TILE + 1)
    chosen = jax.random.randint(second_key, (), 0, LEAVES)
    return jnp.where(jnp.arange(LEAVES) == chosen, WL // TILE, drawn).astype(jnp.int32)


def draw_coupled(key, part):
    leaf_keys = jax.random.split(jax.random.fold_in(key, 23), LEAVES)

    def one_leaf(leaf_key):
        return jax.random.permutation(leaf_key, ANC_TILES)[:NCT]
    return jax.vmap(one_leaf)(leaf_keys).astype(jnp.int32)


def block_levels(stream_key, dims, cuts, low, top_value):
    def one(axis_at, blocks):
        steps = jax.random.uniform(jax.random.fold_in(jax.random.fold_in(stream_key, 6), axis_at), (blocks,), jnp.float32, low / len(cuts), top_value / len(cuts))
        return jnp.repeat(jnp.exp(steps), dims[axis_at] // blocks).reshape((-1,) + (1,) * (len(dims) - axis_at - 1))

    loudness = one(*cuts[0])
    for cut in cuts[1:]:
        loudness = loudness * one(*cut)
    return loudness


def bell_draw(key, dims, scale, most, shards=(), held_as=jnp.bfloat16):
    entries = scale * jax.random.normal(key, dims, jnp.float32)
    if shards:
        entries = entries * block_levels(key, dims, shards, -0.22, 0.18)
    return jnp.clip(entries, -most, most).astype(held_as)


def setup_inputs(seed: int = 0) -> dict:
    splits = jax.random.split(jax.random.key(seed), 13)
    leaf_probe = bell_draw(splits[0], (LEAVES, WL, COLS), 1.0, 6.0, ((0, 128),))
    leaf_lower_inv = bell_draw(splits[1], (LEAVES, WL, WL), WL ** -0.5, 0.25, ((0, 128),))
    leaf_upper_inv = bell_draw(splits[2], (LEAVES, WL, WL), WL ** -0.5, 0.25, ((0, 128),))
    leaf_lower_panel = bell_draw(splits[3], (LEAVES, NCT * TILE, WL), (WL * LEAVES * NCT // ANC_TILES) ** -0.5, 0.09375, ((0, 128),))
    leaf_upper_panel = bell_draw(splits[4], (LEAVES, WL, NCT * TILE), (NCT * TILE) ** -0.5, 0.1875, ((0, 128),))
    leaf_tiles = draw_leaf_tiles(jax.random.fold_in(splits[12], 71), 0)
    coupled = draw_coupled(jax.random.fold_in(splits[12], 71), 0)
    top_probe = bell_draw(splits[7], (LEVELS, SEP, COLS), 1.0, 6.0, ((1, 32),))
    top_lower_inv = bell_draw(splits[8], (LEVELS, SEP, SEP), SEP ** -0.5, 0.09375, ((1, 32),))
    top_lower_blocks = bell_draw(splits[9], (PAIRS, SEP, SEP), (2 * SEP) ** -0.5, 0.0625, ((1, 32),))
    top_upper_inv = bell_draw(splits[10], (LEVELS, SEP, SEP), SEP ** -0.5, 0.09375, ((1, 32),))
    top_upper_blocks = bell_draw(splits[11], (PAIRS, SEP, SEP), (2 * SEP) ** -0.5, 0.0625, ((1, 32),))
    return dict(leaf_probe=leaf_probe, leaf_lower_inv=leaf_lower_inv, leaf_upper_inv=leaf_upper_inv, leaf_lower_panel=leaf_lower_panel, leaf_upper_panel=leaf_upper_panel, leaf_tiles=leaf_tiles, coupled=coupled, top_probe=top_probe, top_lower_inv=top_lower_inv, top_lower_blocks=top_lower_blocks, top_upper_inv=top_upper_inv, top_upper_blocks=top_upper_blocks)


def pair_index(higher, lower):
    return higher * (higher - 1) // 2 + lower


def reference(leaf_probe, leaf_lower_inv, leaf_upper_inv, leaf_lower_panel, leaf_upper_panel, leaf_tiles, coupled, top_probe, top_lower_inv, top_lower_blocks, top_upper_inv, top_upper_blocks):
    row_index = jnp.arange(WL, dtype=jnp.int32)

    def forward_leaf(leaf_item):
        probe_part, inverse_part, panel_part, live_tiles = leaf_item
        live_mask = (row_index < live_tiles * TILE)[:, None]
        masked = jnp.where(live_mask, probe_part, jnp.zeros_like(probe_part))
        solved = jnp.where(live_mask, jnp.dot(inverse_part, masked, preferred_element_type=jnp.float32), 0.0).astype(jnp.bfloat16)
        return solved, jnp.dot(panel_part, solved, preferred_element_type=jnp.float32)

    leaf_forward, contribution = lax.map(forward_leaf, (leaf_probe, leaf_lower_inv, leaf_lower_panel, leaf_tiles))
    update = jnp.zeros((ANC_TILES, TILE, COLS), jnp.float32)
    update = update.at[coupled.reshape(-1)].add(contribution.reshape(-1, TILE, COLS))
    update = update.reshape(LEVELS, SEP, COLS)
    forward_levels = []
    for level in range(LEVELS):
        target = top_probe[level].astype(jnp.float32) - update[level]
        for other in range(level):
            target = target - jnp.dot(top_lower_blocks[pair_index(level, other)], forward_levels[other], preferred_element_type=jnp.float32)
        target = target.astype(jnp.bfloat16)
        forward_levels.append(jnp.dot(top_lower_inv[level], target, preferred_element_type=jnp.float32).astype(jnp.bfloat16))
    solutions = [None] * LEVELS
    rounded = [None] * LEVELS
    for level in range(LEVELS - 1, -1, -1):
        target = forward_levels[level].astype(jnp.float32)
        for other in range(LEVELS - 1, level, -1):
            target = target - jnp.dot(top_upper_blocks[pair_index(other, level)], rounded[other], preferred_element_type=jnp.float32)
        target = target.astype(jnp.bfloat16)
        solutions[level] = jnp.dot(top_upper_inv[level], target, preferred_element_type=jnp.float32)
        rounded[level] = solutions[level].astype(jnp.bfloat16)
    whole_top = jnp.stack(rounded).reshape(ANC_TILES, TILE, COLS)

    def backward_leaf(leaf_item):
        forward_part, inverse_part, panel_part, live_tiles, blocks = leaf_item
        live_mask = (row_index < live_tiles * TILE)[:, None]
        picked = whole_top[blocks].reshape(NCT * TILE, COLS)
        target = forward_part.astype(jnp.float32) - jnp.dot(panel_part, picked, preferred_element_type=jnp.float32)
        target = jnp.where(live_mask, target, 0.0).astype(jnp.bfloat16)
        return jnp.where(live_mask, jnp.dot(inverse_part, target, preferred_element_type=jnp.float32), 0.0)

    leaf_solution = lax.map(backward_leaf, (leaf_forward, leaf_upper_inv, leaf_upper_panel, leaf_tiles, coupled))
    return leaf_solution, jnp.stack(solutions)
```

```python
import jax
import jax.numpy as jnp
from jax import lax
from jax.experimental import pallas as pl
from jax.experimental.pallas import tpu as pltpu
from jax.sharding import Mesh
from jax.sharding import PartitionSpec as P


TILE = 128
ROW_COL = ("row_0", "row_1", "col")
GZ_ROW_COL = ("gz", "row_0", "row_1", "col")
CHIPS = ("row_0", "col")
SLICES = ("gz", "row_1")
SWAP = [(0, 1), (1, 0)]
NT = (((1,), (1,)), ((), ()))
BF16 = jnp.bfloat16
F32 = jnp.float32


def pair_index(higher, lower):
    return higher * (higher - 1) // 2 + lower


def params(mebibytes):
    return pltpu.CompilerParams(vmem_limit_bytes=int(mebibytes * 2**20))


def vmem():
    return pl.BlockSpec(memory_space=pltpu.VMEM)


def smem():
    return pl.BlockSpec(memory_space=pltpu.SMEM)


def anywhere():
    return pl.BlockSpec(memory_space=pl.ANY)


def hbm():
    return pl.BlockSpec(memory_space=pltpu.HBM)


def live_mask(tiles_ref, rows, columns):
    return lax.broadcasted_iota(jnp.int32, (rows, columns), 0) < tiles_ref[0] * TILE


def leaf_forward(tiles, coupled, probe, inverse, panel):
    rows, columns = probe.shape[1:]
    blocks = coupled.shape[1]
    panel_rows = panel.shape[1]

    def kernel(
        tiles_ref, coupled_ref, probe_ref, inverse_ref, panel_ref, out_ref, solved_ref, pr, iv, pn, sems
    ):
        copies = [
            pltpu.make_async_copy(probe_ref.at[0], pr, sems.at[0]),
            pltpu.make_async_copy(inverse_ref.at[0], iv, sems.at[1]),
            pltpu.make_async_copy(panel_ref.at[0], pn, sems.at[2]),
        ]
        for copy in copies:
            copy.start()
        live = live_mask(tiles_ref, rows, columns)
        lane = lax.broadcasted_iota(jnp.int32, (columns, TILE), 1)
        ids = jnp.zeros((columns, TILE), F32)
        for j in range(blocks):
            ids = jnp.where(lane == j, coupled_ref[0, j].astype(F32), ids)
        out_ref[:, panel_rows:] = ids.astype(BF16)
        copies[0].wait()
        masked = jnp.where(live, pr[...], jnp.zeros((rows, columns), BF16))
        copies[1].wait()
        solved = jnp.dot(iv[...], masked, preferred_element_type=F32)
        solved = jnp.where(live, solved, 0.0)
        solved_ref[...] = solved.astype(BF16)
        turned = solved.T.astype(BF16)
        copies[2].wait()
        out_ref[:, :panel_rows] = lax.dot_general(
            turned, pn[...], NT, preferred_element_type=F32
        ).astype(BF16)

    return pl.pallas_call(
        kernel,
        out_shape=(
            jax.ShapeDtypeStruct((columns, panel_rows + TILE), BF16),
            jax.ShapeDtypeStruct((rows, columns), BF16),
        ),
        in_specs=[smem(), smem(), hbm(), hbm(), hbm()],
        out_specs=(vmem(), vmem()),
        scratch_shapes=[
            pltpu.VMEM((rows, columns), BF16),
            pltpu.VMEM((rows, rows), BF16),
            pltpu.VMEM((panel_rows, rows), BF16),
            pltpu.SemaphoreType.DMA((3,)),
        ],
        compiler_params=params(50),
        name="leaf_forward",
    )(tiles, coupled, probe, inverse, panel)


def block_place(block, chip_cols):
    per_chip_row = 2 * chip_cols
    in_level = block % (per_chip_row * (32 // per_chip_row))
    chip = in_level // per_chip_row * chip_cols + in_level % chip_cols
    core = in_level % per_chip_row // chip_cols
    return block // 32, chip, core


def scatter_update(exchanged, levels):
    peers, width, _ = exchanged.shape
    blocks = 8
    data = blocks * TILE

    def kernel(ex_ref, out_ref, ids_ref, dense, ids_s, sem):
        ids_ref[...] = ex_ref[:, 0, data:].astype(F32).astype(jnp.int32)
        copy = pltpu.make_async_copy(ids_ref, ids_s, sem)
        copy.start()
        dense[...] = jnp.zeros(dense.shape, F32)
        copy.wait()
        for p in range(peers):
            for j in range(blocks):
                b = ids_s[p, j]
                dense[b] += ex_ref[p, :, j * TILE : (j + 1) * TILE].astype(F32)
        for b in range(levels * 32):
            level, chip, core = block_place(b, 4)
            out_ref[chip, level, :, core * TILE : (core + 1) * TILE] = dense[b].astype(BF16)

    return pl.pallas_call(
        kernel,
        out_shape=(
            jax.ShapeDtypeStruct((16, levels, width, 2 * TILE), BF16),
            jax.ShapeDtypeStruct((peers, TILE), jnp.int32),
        ),
        in_specs=[vmem()],
        out_specs=(vmem(), vmem()),
        scratch_shapes=[
            pltpu.VMEM((levels * 32, width, TILE), F32),
            pltpu.SMEM((peers, TILE), jnp.int32),
            pltpu.SemaphoreType.DMA,
        ],
        compiler_params=params(4),
        name="scatter_update",
    )(exchanged)


def probe_rows(after, place, own, partner, width):
    levels, rows, columns = own.shape

    def kernel(after_ref, place_ref, own_ref, partner_ref, out_ref, turned):
        first = place_ref[0] == 0
        start = pl.multiple_of(place_ref[1] * width, width)
        for level in range(levels):
            for k, ref in enumerate((own_ref, partner_ref)):
                turned[k] = ref[level].astype(F32).T
            mine = turned[0, pl.ds(start, width), :]
            other = turned[1, pl.ds(start, width), :]
            out_ref[level, :, :rows] = jnp.where(first, mine, other)
            out_ref[level, :, rows:] = jnp.where(first, other, mine)

    return pl.pallas_call(
        kernel,
        out_shape=jax.ShapeDtypeStruct((levels, width, 2 * rows), F32),
        in_specs=[anywhere(), smem(), vmem(), vmem()],
        out_specs=vmem(),
        scratch_shapes=[pltpu.VMEM((2, columns, rows), F32)],
        compiler_params=params(3),
        name="probe_rows",
    )(after, place, own, partner)


def reduce_update(received, probe):
    chips, levels, width, rows = received.shape

    def kernel(rec_ref, probe_ref, first_ref, rest_ref):
        for level in range(levels):
            total = rec_ref[0, level].astype(F32)
            for chip in range(1, chips):
                total = total + rec_ref[chip, level].astype(F32)
            target = probe_ref[level].astype(F32) - total
            if level == 0:
                first_ref[...] = jnp.broadcast_to(target.astype(BF16)[None], first_ref.shape)
            else:
                rest_ref[level - 1] = target

    return pl.pallas_call(
        kernel,
        out_shape=(
            jax.ShapeDtypeStruct((chips, width, rows), BF16),
            jax.ShapeDtypeStruct((levels - 1, width, rows), F32),
        ),
        in_specs=[vmem(), vmem()],
        out_specs=(vmem(), vmem()),
        compiler_params=params(3),
        name="reduce_update",
    )(received, probe)


def load_rows(after, own, partner, index):
    rows, sep = own.shape[1:]

    def kernel(after_ref, own_ref, partner_ref, out_ref, sems):
        copies = [
            pltpu.make_async_copy(own_ref.at[index], out_ref.at[0], sems.at[0]),
            pltpu.make_async_copy(partner_ref.at[index], out_ref.at[1], sems.at[1]),
        ]
        for copy in copies:
            copy.start()
        for copy in copies:
            copy.wait()

    return pl.pallas_call(
        kernel,
        out_shape=jax.ShapeDtypeStruct((2, rows, sep), BF16),
        in_specs=[anywhere(), hbm(), hbm()],
        out_specs=vmem(),
        scratch_shapes=[pltpu.SemaphoreType.DMA((2,))],
        compiler_params=params(50),
        name="load_rows",
    )(after, own, partner)


def products(core_ref, g_ref, first_weights, second_weights):
    parts = []
    for z in range(4):
        for c in range(2):
            for y in range(4):
                parts.append(g_ref[z * 4 + y, :, c * TILE : (c + 1) * TILE])
    whole = jnp.concatenate(parts, 1)
    mine = lax.dot_general(whole, first_weights(), NT, preferred_element_type=F32)
    other = lax.dot_general(whole, second_weights(), NT, preferred_element_type=F32)
    first = core_ref[0] == 0
    return jnp.where(first, mine, other), jnp.where(first, other, mine)


def apply_loaded(core, gathered, weights, base):
    chips, width, rows = gathered.shape

    def kernel(core_ref, g_ref, w_ref, *refs):
        halves = products(core_ref, g_ref, lambda: w_ref[0], lambda: w_ref[1])
        out_ref = refs[-1]
        for k, half in enumerate(halves):
            lanes = slice(k * TILE, (k + 1) * TILE)
            if base is not None:
                base_ref = refs[0]
                start = base_ref[0][:, lanes] if base.ndim == 3 else base_ref[:, lanes]
                half = start.astype(F32) - half
            out_ref[:, :, lanes] = jnp.broadcast_to(half.astype(BF16)[None], (chips, width, TILE))

    operands = [gathered, weights] + ([] if base is None else [base])
    return pl.pallas_call(
        kernel,
        out_shape=pltpu.VMEM((chips, width, rows), BF16),
        in_specs=[smem()] + [vmem()] * len(operands),
        out_specs=vmem(),
        compiler_params=params(4),
        name="apply_loaded",
    )(core, *operands)


def subtract_rows(core, gathered, own, partner, index, base):
    _, width, rows = gathered.shape
    sep = own.shape[2]

    def kernel(core_ref, g_ref, own_ref, partner_ref, base_ref, out_ref, w, sems):
        copies = [
            pltpu.make_async_copy(own_ref.at[index], w.at[0], sems.at[0]),
            pltpu.make_async_copy(partner_ref.at[index], w.at[1], sems.at[1]),
        ]
        for copy in copies:
            copy.start()

        def arrived(k):
            copies[k].wait()
            return w[k]

        halves = products(core_ref, g_ref, lambda: arrived(0), lambda: arrived(1))
        for k, half in enumerate(halves):
            lanes = slice(k * TILE, (k + 1) * TILE)
            start = base_ref[0][:, lanes] if base.ndim == 3 else base_ref[:, lanes]
            out_ref[:, lanes] = start.astype(F32) - half

    return pl.pallas_call(
        kernel,
        out_shape=jax.ShapeDtypeStruct((width, rows), F32),
        in_specs=[smem(), vmem(), hbm(), hbm(), vmem()],
        out_specs=vmem(),
        scratch_shapes=[pltpu.VMEM((2, TILE, sep), BF16), pltpu.SemaphoreType.DMA((2,))],
        compiler_params=params(50),
        name="subtract_rows",
    )(core, gathered, own, partner, base)


def pick_blocks(ids, wholes, owns):
    levels = len(wholes)
    _, width, _ = wholes[0].shape
    peers = ids.shape[0]
    blocks = 8

    def kernel(*refs):
        ids_ref = refs[0]
        whole_refs = refs[1 : 1 + levels]
        own_refs = refs[1 + levels : 1 + 2 * levels]
        out_ref, every, ids_s, sem = refs[1 + 2 * levels :]
        copy = pltpu.make_async_copy(ids_ref, ids_s, sem)
        copy.start()
        for b in range(levels * 32):
            level, chip, core = block_place(b, 4)
            every[b] = whole_refs[level][chip, :, core * TILE : (core + 1) * TILE]
        for p in range(peers):
            core = p % 2
            for level in range(levels):
                start = (blocks + level) * TILE
                out_ref[p, :, start : start + TILE] = own_refs[level][
                    0, :, core * TILE : (core + 1) * TILE
                ]
        copy.wait()
        for p in range(peers):
            for j in range(blocks):
                out_ref[p, :, j * TILE : (j + 1) * TILE] = every[ids_s[p, j]]

    return pl.pallas_call(
        kernel,
        out_shape=jax.ShapeDtypeStruct((peers, width, (blocks + levels) * TILE), BF16),
        in_specs=[vmem()] * (1 + 2 * levels),
        out_specs=vmem(),
        scratch_shapes=[
            pltpu.VMEM((levels * 32, width, TILE), BF16),
            pltpu.SMEM((peers, TILE), jnp.int32),
            pltpu.SemaphoreType.DMA,
        ],
        compiler_params=params(4),
        name="pick_blocks",
    )(ids, *wholes, *owns)


def leaf_backward(tiles, picked, panel, inverse, solved, levels):
    rows, columns = solved.shape
    panel_columns = panel.shape[2]

    def kernel(tiles_ref, picked_ref, panel_ref, inverse_ref, solved_ref, leaf_ref, top_ref):
        live = live_mask(tiles_ref, rows, columns)
        product = lax.dot_general(
            panel_ref[0], picked_ref[:, :panel_columns], NT, preferred_element_type=F32
        )
        target = jnp.where(live, solved_ref[...].astype(F32) - product, 0.0).astype(BF16)
        solution = jnp.dot(inverse_ref[0], target, preferred_element_type=F32)
        leaf_ref[0] = jnp.where(live, solution, 0.0)
        for level in range(levels):
            start = panel_columns + level * TILE
            top_ref[level] = picked_ref[:, start : start + TILE].astype(F32).T

    return pl.pallas_call(
        kernel,
        out_shape=(
            jax.ShapeDtypeStruct((1, rows, columns), F32),
            jax.ShapeDtypeStruct((levels, TILE, columns), F32),
        ),
        in_specs=[smem(), vmem(), vmem(), vmem(), vmem()],
        out_specs=(vmem(), vmem()),
        compiler_params=params(5),
        name="leaf_backward",
    )(tiles, picked, panel, inverse, solved)


def exchange(array, axes):
    return lax.all_to_all(array, axes, 0, 0, tiled=True)


def body(
    leaf_probe,
    leaf_lower_inv,
    leaf_upper_inv,
    leaf_lower_panel,
    leaf_upper_panel,
    leaf_tiles,
    coupled,
    top_probe,
    top_lower_inv,
    top_lower_blocks,
    top_upper_inv,
    top_upper_blocks,
):
    levels = top_probe.shape[0]
    columns = leaf_probe.shape[2]
    peers = lax.axis_size(SLICES)
    width = columns // peers
    core = lax.axis_index("row_1").astype(jnp.int32).reshape(1)
    slice_index = lax.axis_index(SLICES)

    probe_p = lax.ppermute(top_probe, "row_1", SWAP)
    lower_inv_p = lax.ppermute(top_lower_inv, "row_1", SWAP)
    lower_blocks_p = lax.ppermute(top_lower_blocks, "row_1", SWAP)
    lower = [(top_lower_inv, lower_inv_p), (top_lower_blocks, lower_blocks_p)]
    place = jnp.concatenate([core, slice_index.astype(jnp.int32).reshape(1)])

    sent, solved = leaf_forward(
        leaf_tiles, coupled, leaf_probe, leaf_lower_inv, leaf_lower_panel
    )
    exchanged = exchange(sent.reshape(peers, width, -1), SLICES)
    dense, ids = scatter_update(exchanged, levels)
    weights = load_rows(dense, *lower[0], 0)
    probe = probe_rows(dense, place, top_probe, probe_p, width)
    received = exchange(dense, CHIPS)
    target, rest = reduce_update(received, probe)
    partial = [None] + [rest[a] for a in range(levels - 1)]
    solved_top = []
    for level in range(levels):
        if level > 0:
            weights = load_rows(target, *lower[0], level)
        whole = exchange(target, CHIPS)
        mine = apply_loaded(core, whole, weights, None)
        solved_top.append(mine)
        if level + 1 < levels:
            weights = load_rows(mine, *lower[1], pair_index(level + 1, level))
            whole = exchange(mine, CHIPS)
            target = apply_loaded(core, whole, weights, partial[level + 1])
            if level == 0:
                upper_in, target = lax.optimization_barrier(
                    ((top_upper_inv, top_upper_blocks), target)
                )
                upper = [(array, lax.ppermute(array, "row_1", SWAP)) for array in upper_in]
            for higher in range(level + 2, levels):
                partial[higher] = subtract_rows(
                    core, whole, *lower[1], pair_index(higher, level), partial[higher]
                )
    target = solved_top[levels - 1]
    partial = list(solved_top)
    wholes = [None] * levels
    owns = [None] * levels
    for level in range(levels - 1, -1, -1):
        weights = load_rows(target, *upper[0], level)
        whole = exchange(target, CHIPS)
        owns[level] = apply_loaded(core, whole, weights, None)
        if level > 0:
            weights = load_rows(owns[level], *upper[1], pair_index(level, level - 1))
        whole = exchange(owns[level], CHIPS)
        wholes[level] = whole
        if level > 0:
            target = apply_loaded(core, whole, weights, partial[level - 1])
            for lower_level in range(level - 2, -1, -1):
                partial[lower_level] = subtract_rows(
                    core,
                    whole,
                    *upper[1],
                    pair_index(level, lower_level),
                    partial[lower_level],
                )
    picked = exchange(pick_blocks(ids, wholes, owns), SLICES)
    return leaf_backward(
        leaf_tiles,
        picked.reshape(columns, -1),
        leaf_upper_panel,
        leaf_upper_inv,
        solved,
        levels,
    )


def solution(mesh):
    finer = Mesh(
        mesh.devices.reshape(mesh.shape["gz"], 4, 2, mesh.shape["col"]),
        ("gz", "row_0", "row_1", "col"),
    )
    in_specs = (
        P(GZ_ROW_COL, None, None),
        P(GZ_ROW_COL, None, None),
        P(GZ_ROW_COL, None, None),
        P(GZ_ROW_COL, None, None),
        P(GZ_ROW_COL, None, None),
        P(GZ_ROW_COL),
        P(GZ_ROW_COL, None),
        P(None, ROW_COL, None),
        P(None, ROW_COL, None),
        P(None, ROW_COL, None),
        P(None, ROW_COL, None),
        P(None, ROW_COL, None),
    )
    out_specs = (P(GZ_ROW_COL, None, None), P(None, ROW_COL, None))

    return jax.shard_map(
        body, mesh=finer, in_specs=in_specs, out_specs=out_specs, check_vma=False
    )
```

```python
import jax
import jax.numpy as jnp
from jax import lax
from jax.experimental import pallas as pl
from jax.experimental.pallas import tpu as pltpu
from jax.sharding import Mesh
from jax.sharding import PartitionSpec as P


TILE = 128
ROW_COL = ("row_0", "row_1", "col")
GZ_ROW_COL = ("gz", "row_0", "row_1", "col")
CHIPS = ("row_0", "col")
SLICES = ("gz", "row_1")
SWAP = [(0, 1), (1, 0)]
NT = (((1,), (1,)), ((), ()))
BF16 = jnp.bfloat16
F32 = jnp.float32


def pair_index(higher, lower):
    return higher * (higher - 1) // 2 + lower


def params(mebibytes):
    return pltpu.CompilerParams(vmem_limit_bytes=int(mebibytes * 2**20))


def vmem():
    return pl.BlockSpec(memory_space=pltpu.VMEM)


def smem():
    return pl.BlockSpec(memory_space=pltpu.SMEM)


def anywhere():
    return pl.BlockSpec(memory_space=pl.ANY)


def hbm():
    return pl.BlockSpec(memory_space=pltpu.HBM)


def live_mask(tiles_ref, rows, columns):
    return lax.broadcasted_iota(jnp.int32, (rows, columns), 0) < tiles_ref[0] * TILE


def row_copies(source, target, sems, first, pieces):
    rows = target.shape[0] // pieces
    return [
        pltpu.make_async_copy(
            source.at[pl.ds(k * rows, rows)], target.at[pl.ds(k * rows, rows)], sems.at[first + k]
        )
        for k in range(pieces)
    ]


def leaf_forward(place, tiles, coupled, probe, inverse, panel, top_probe, width):
    rows, columns = probe.shape[1:]
    blocks = coupled.shape[1]
    panel_rows = panel.shape[1]
    levels, top_rows, _ = top_probe.shape

    def kernel(
        place_ref,
        tiles_ref,
        coupled_ref,
        probe_ref,
        inverse_ref,
        panel_ref,
        top_ref,
        out_ref,
        solved_ref,
        mine_ref,
        other_ref,
        pr,
        iv,
        pn,
        tp,
        turned,
        sems,
    ):
        probe_copy = pltpu.make_async_copy(probe_ref.at[0], pr, sems.at[0])
        top_copy = pltpu.make_async_copy(top_ref, tp, sems.at[1])
        inverse_copies = row_copies(inverse_ref.at[0], iv, sems, 2, 4)
        panel_copies = row_copies(panel_ref.at[0], pn, sems, 6, 4)
        for copy in [top_copy, probe_copy] + inverse_copies + panel_copies:
            copy.start()
        live = live_mask(tiles_ref, rows, columns)
        lane = lax.broadcasted_iota(jnp.int32, (columns, TILE), 1)
        ids = jnp.zeros((columns, TILE), F32)
        for j in range(blocks):
            ids = jnp.where(lane == j, coupled_ref[0, j].astype(F32), ids)
        out_ref[:, panel_rows:] = ids.astype(BF16)
        here = place_ref[0]
        there = here + 1 - 2 * lax.rem(here, 2)
        top_copy.wait()
        for level in range(levels):
            turned[level] = tp[level].astype(F32).T
        for index, ref in ((here, mine_ref), (there, other_ref)):
            start = pl.multiple_of(index * width, width)
            for level in range(levels):
                ref[level] = turned[level, pl.ds(start, width), :].astype(BF16)
        probe_copy.wait()
        masked = jnp.where(live, pr[...], jnp.zeros((rows, columns), BF16))
        for copy in inverse_copies:
            copy.wait()
        solved = jnp.dot(iv[...], masked, preferred_element_type=F32)
        solved = jnp.where(live, solved, 0.0)
        solved_ref[...] = solved.astype(BF16)
        across = solved.T.astype(BF16)
        for copy in panel_copies:
            copy.wait()
        out_ref[:, :panel_rows] = lax.dot_general(
            across, pn[...], NT, preferred_element_type=F32
        ).astype(BF16)

    return pl.pallas_call(
        kernel,
        out_shape=(
            jax.ShapeDtypeStruct((columns, panel_rows + TILE), BF16),
            jax.ShapeDtypeStruct((rows, columns), BF16),
            jax.ShapeDtypeStruct((levels, width, top_rows), BF16),
            jax.ShapeDtypeStruct((levels, width, top_rows), BF16),
        ),
        in_specs=[smem(), smem(), smem(), hbm(), hbm(), hbm(), hbm()],
        out_specs=(vmem(), vmem(), vmem(), vmem()),
        scratch_shapes=[
            pltpu.VMEM((rows, columns), BF16),
            pltpu.VMEM((rows, rows), BF16),
            pltpu.VMEM((panel_rows, rows), BF16),
            pltpu.VMEM((levels, top_rows, columns), BF16),
            pltpu.VMEM((levels, columns, top_rows), F32),
            pltpu.SemaphoreType.DMA((10,)),
        ],
        compiler_params=params(63),
        name="leaf_forward",
    )(place, tiles, coupled, probe, inverse, panel, top_probe)


def block_place(block, chip_cols):
    per_chip_row = 2 * chip_cols
    in_level = block % (per_chip_row * (32 // per_chip_row))
    chip = in_level // per_chip_row * chip_cols + in_level % chip_cols
    core = in_level % per_chip_row // chip_cols
    return block // 32, chip, core


def scatter_update(exchanged, levels):
    peers, width, _ = exchanged.shape
    blocks = 8
    data = blocks * TILE

    def kernel(ex_ref, out_ref, ids_ref, dense, ids_s, sem):
        ids_ref[...] = ex_ref[:, 0, data:].astype(F32).astype(jnp.int32)
        copy = pltpu.make_async_copy(ids_ref, ids_s, sem)
        copy.start()
        dense[...] = jnp.zeros(dense.shape, F32)
        copy.wait()
        for p in range(peers):
            for j in range(blocks):
                b = ids_s[p, j]
                dense[b] += ex_ref[p, :, j * TILE : (j + 1) * TILE].astype(F32)
        for b in range(levels * 32):
            level, chip, core = block_place(b, 4)
            out_ref[chip, level, :, core * TILE : (core + 1) * TILE] = dense[b].astype(BF16)

    return pl.pallas_call(
        kernel,
        out_shape=(
            jax.ShapeDtypeStruct((16, levels, width, 2 * TILE), BF16),
            jax.ShapeDtypeStruct((peers, TILE), jnp.int32),
        ),
        in_specs=[vmem()],
        out_specs=(vmem(), vmem()),
        scratch_shapes=[
            pltpu.VMEM((levels * 32, width, TILE), F32),
            pltpu.SMEM((peers, TILE), jnp.int32),
            pltpu.SemaphoreType.DMA,
        ],
        compiler_params=params(4),
        name="scatter_update",
    )(exchanged)


def reduce_update(place, received, mine, other):
    chips, levels, width, rows = received.shape

    def kernel(place_ref, rec_ref, mine_ref, other_ref, first_ref, *rest_refs):
        low_first = lax.rem(place_ref[0], 2) == 0
        for level in range(levels):
            total = rec_ref[0, level].astype(F32)
            for chip in range(1, chips):
                total = total + rec_ref[chip, level].astype(F32)
            own, partner = mine_ref[level].astype(F32), other_ref[level].astype(F32)
            low = jnp.where(low_first, own, partner)
            high = jnp.where(low_first, partner, own)
            target = jnp.concatenate([low, high], 1) - total
            if level == 0:
                first_ref[...] = jnp.broadcast_to(target.astype(BF16)[None], first_ref.shape)
            else:
                rest_refs[level - 1][...] = target

    return pl.pallas_call(
        kernel,
        out_shape=(jax.ShapeDtypeStruct((chips, width, rows), BF16),)
        + (jax.ShapeDtypeStruct((width, rows), F32),) * (levels - 1),
        in_specs=[smem(), vmem(), vmem(), vmem()],
        out_specs=(vmem(),) * levels,
        compiler_params=params(3),
        name="reduce_update",
    )(place, received, mine, other)


def load_rows(after, own, partner, index):
    rows, sep = own.shape[1:]

    def kernel(after_ref, own_ref, partner_ref, out_ref, sems):
        copies = row_copies(own_ref.at[index], out_ref.at[0], sems, 0, 4)
        copies += row_copies(partner_ref.at[index], out_ref.at[1], sems, 4, 4)
        for copy in copies:
            copy.start()
        for copy in copies:
            copy.wait()

    return pl.pallas_call(
        kernel,
        out_shape=jax.ShapeDtypeStruct((2, rows, sep), BF16),
        in_specs=[anywhere(), hbm(), hbm()],
        out_specs=vmem(),
        scratch_shapes=[pltpu.SemaphoreType.DMA((8,))],
        compiler_params=params(50),
        name="load_rows",
    )(after, own, partner)


def products(core_ref, g_ref, first_weights, second_weights):
    parts = []
    for z in range(4):
        for c in range(2):
            for y in range(4):
                parts.append(g_ref[z * 4 + y, :, c * TILE : (c + 1) * TILE])
    whole = jnp.concatenate(parts, 1)
    mine = lax.dot_general(whole, first_weights(), NT, preferred_element_type=F32)
    other = lax.dot_general(whole, second_weights(), NT, preferred_element_type=F32)
    first = lax.rem(core_ref[0], 2) == 0
    return jnp.where(first, mine, other), jnp.where(first, other, mine)


def apply_loaded(core, gathered, weights, base):
    chips, width, rows = gathered.shape

    def kernel(core_ref, g_ref, w_ref, *refs):
        halves = products(core_ref, g_ref, lambda: w_ref[0], lambda: w_ref[1])
        out_ref = refs[-1]
        for k, half in enumerate(halves):
            lanes = slice(k * TILE, (k + 1) * TILE)
            if base is not None:
                base_ref = refs[0]
                start = base_ref[0][:, lanes] if base.ndim == 3 else base_ref[:, lanes]
                half = start.astype(F32) - half
            out_ref[:, :, lanes] = jnp.broadcast_to(half.astype(BF16)[None], (chips, width, TILE))

    operands = [gathered, weights] + ([] if base is None else [base])
    return pl.pallas_call(
        kernel,
        out_shape=pltpu.VMEM((chips, width, rows), BF16),
        in_specs=[smem()] + [vmem()] * len(operands),
        out_specs=vmem(),
        compiler_params=params(4),
        name="apply_loaded",
    )(core, *operands)


def subtract_rows(after, core, gathered, own, partner, index, base):
    _, width, rows = gathered.shape
    sep = own.shape[2]

    def kernel(after_ref, core_ref, g_ref, own_ref, partner_ref, base_ref, out_ref, w, sems):
        copies = [
            row_copies(own_ref.at[index], w.at[0], sems, 0, 4),
            row_copies(partner_ref.at[index], w.at[1], sems, 4, 4),
        ]
        for copy in copies[0] + copies[1]:
            copy.start()

        def arrived(k):
            for copy in copies[k]:
                copy.wait()
            return w[k]

        halves = products(core_ref, g_ref, lambda: arrived(0), lambda: arrived(1))
        for k, half in enumerate(halves):
            lanes = slice(k * TILE, (k + 1) * TILE)
            start = base_ref[0][:, lanes] if base.ndim == 3 else base_ref[:, lanes]
            out_ref[:, lanes] = start.astype(F32) - half

    return pl.pallas_call(
        kernel,
        out_shape=jax.ShapeDtypeStruct((width, rows), F32),
        in_specs=[anywhere(), smem(), vmem(), hbm(), hbm(), vmem()],
        out_specs=vmem(),
        scratch_shapes=[pltpu.VMEM((2, TILE, sep), BF16), pltpu.SemaphoreType.DMA((8,))],
        compiler_params=params(50),
        name="subtract_rows",
    )(after, core, gathered, own, partner, base)


def pick_blocks(ids, wholes, owns):
    levels = len(wholes)
    _, width, _ = wholes[0].shape
    peers = ids.shape[0]
    blocks = 8

    def kernel(*refs):
        ids_ref = refs[0]
        whole_refs = refs[1 : 1 + levels]
        own_refs = refs[1 + levels : 1 + 2 * levels]
        out_ref, every, ids_s, sem = refs[1 + 2 * levels :]
        copy = pltpu.make_async_copy(ids_ref, ids_s, sem)
        copy.start()
        for b in range(levels * 32):
            level, chip, core = block_place(b, 4)
            every[b] = whole_refs[level][chip, :, core * TILE : (core + 1) * TILE]
        for p in range(peers):
            core = p % 2
            for level in range(levels):
                start = (blocks + level) * TILE
                out_ref[p, :, start : start + TILE] = own_refs[level][
                    0, :, core * TILE : (core + 1) * TILE
                ]
        copy.wait()
        for p in range(peers):
            for j in range(blocks):
                out_ref[p, :, j * TILE : (j + 1) * TILE] = every[ids_s[p, j]]

    return pl.pallas_call(
        kernel,
        out_shape=jax.ShapeDtypeStruct((peers, width, (blocks + levels) * TILE), BF16),
        in_specs=[vmem()] * (1 + 2 * levels),
        out_specs=vmem(),
        scratch_shapes=[
            pltpu.VMEM((levels * 32, width, TILE), BF16),
            pltpu.SMEM((peers, TILE), jnp.int32),
            pltpu.SemaphoreType.DMA,
        ],
        compiler_params=params(4),
        name="pick_blocks",
    )(ids, *wholes, *owns)


def leaf_backward(tiles, picked, panel, inverse, solved, levels):
    rows, columns = solved.shape
    panel_columns = panel.shape[2]

    def kernel(tiles_ref, picked_ref, panel_ref, inverse_ref, solved_ref, leaf_ref, top_ref):
        live = live_mask(tiles_ref, rows, columns)
        product = lax.dot_general(
            panel_ref[0], picked_ref[:, :panel_columns], NT, preferred_element_type=F32
        )
        target = jnp.where(live, solved_ref[...].astype(F32) - product, 0.0).astype(BF16)
        solution = jnp.dot(inverse_ref[0], target, preferred_element_type=F32)
        leaf_ref[0] = jnp.where(live, solution, 0.0)
        for level in range(levels):
            start = panel_columns + level * TILE
            top_ref[level] = picked_ref[:, start : start + TILE].astype(F32).T

    return pl.pallas_call(
        kernel,
        out_shape=(
            jax.ShapeDtypeStruct((1, rows, columns), F32),
            jax.ShapeDtypeStruct((levels, TILE, columns), F32),
        ),
        in_specs=[smem(), vmem(), vmem(), vmem(), vmem()],
        out_specs=(vmem(), vmem()),
        compiler_params=params(5),
        name="leaf_backward",
    )(tiles, picked, panel, inverse, solved)


def exchange(array, axes):
    return lax.all_to_all(array, axes, 0, 0, tiled=True)


def body(
    leaf_probe,
    leaf_lower_inv,
    leaf_upper_inv,
    leaf_lower_panel,
    leaf_upper_panel,
    leaf_tiles,
    coupled,
    top_probe,
    top_lower_inv,
    top_lower_blocks,
    top_upper_inv,
    top_upper_blocks,
):
    levels = top_probe.shape[0]
    columns = leaf_probe.shape[2]
    peers = lax.axis_size(SLICES)
    width = columns // peers
    place = lax.axis_index(SLICES).astype(jnp.int32).reshape(1)

    def swapped(array):
        return lax.ppermute(array, "row_1", SWAP)

    lower_inv_p = swapped(top_lower_inv)
    lower_first = top_lower_blocks[:1]
    lower_first_p = swapped(lower_first)
    lower_blocks_p = swapped(top_lower_blocks)
    sent, solved, probe_mine, probe_other = leaf_forward(
        place,
        leaf_tiles,
        coupled,
        leaf_probe,
        leaf_lower_inv,
        leaf_lower_panel,
        top_probe,
        width,
    )
    probe_other = swapped(probe_other)
    exchanged = exchange(sent.reshape(peers, width, -1), SLICES)
    dense, ids = scatter_update(exchanged, levels)
    received = exchange(dense, CHIPS)
    target, *rest = reduce_update(place, received, probe_mine, probe_other)

    lower_inv = (top_lower_inv, lower_inv_p)
    lower_blocks = (top_lower_blocks, lower_blocks_p)
    upper_inv, upper_blocks = None, None
    ready = {}

    def gather(target, loads, subtractions):
        for name, arrays, index in loads:
            ready[name] = load_rows(target, *arrays, index)
        results = {}
        for higher, whole, arrays, index, base in subtractions:
            results[higher] = subtract_rows(target, place, whole, *arrays, index, base)
        whole = exchange(target, CHIPS)
        fresh = [ready[name] for name, _, _ in loads]
        whole, fresh, results = lax.optimization_barrier((whole, fresh, results))
        for (name, _, _), value in zip(loads, fresh):
            ready[name] = value
        return whole, results

    def apply(name, whole, base):
        return apply_loaded(place, whole, ready[name], base)

    t1, t2, t3 = rest
    r0, _ = gather(target, [("f0", lower_inv, 0)], [])
    x0 = apply("f0", r0, None)
    w0, _ = gather(x0, [("f10", (top_lower_blocks, lower_first_p), 0)], [])
    target = apply("f10", w0, t1)
    upper_in, target = lax.optimization_barrier(((top_upper_inv, top_upper_blocks), target))
    upper_inv = (upper_in[0], swapped(upper_in[0]))
    r1, _ = gather(target, [("f1", lower_inv, 1)], [])
    x1 = apply("f1", r1, None)
    upper_next, x1 = lax.optimization_barrier((upper_in[1], x1))
    upper_blocks = (upper_next, swapped(upper_next))
    w1, done = gather(
        x1,
        [("f21", lower_blocks, pair_index(2, 1))],
        [(2, w0, lower_blocks, pair_index(2, 0), t2)],
    )
    target = apply("f21", w1, done[2])
    r2, done = gather(
        target,
        [("f2", lower_inv, 2)],
        [(3, w0, lower_blocks, pair_index(3, 0), t3)],
    )
    t3 = done[3]
    x2 = apply("f2", r2, None)
    w2, done = gather(
        x2,
        [("f32", lower_blocks, pair_index(3, 2))],
        [(3, w1, lower_blocks, pair_index(3, 1), t3)],
    )
    target = apply("f32", w2, done[3])
    r3, _ = gather(target, [("f3", lower_inv, 3)], [])
    x3 = apply("f3", r3, None)

    s3, _ = gather(x3, [("b3", upper_inv, 3)], [])
    y3 = apply("b3", s3, None)
    v3, _ = gather(y3, [("b23", upper_blocks, pair_index(3, 2))], [])
    target = apply("b23", v3, x2)
    s2, done = gather(
        target,
        [("b2", upper_inv, 2)],
        [(1, v3, upper_blocks, pair_index(3, 1), x1)],
    )
    t1 = done[1]
    y2 = apply("b2", s2, None)
    v2, done = gather(
        y2,
        [("b12", upper_blocks, pair_index(2, 1))],
        [(0, v3, upper_blocks, pair_index(3, 0), x0)],
    )
    t0 = done[0]
    target = apply("b12", v2, t1)
    s1, done = gather(
        target,
        [("b1", upper_inv, 1)],
        [(0, v2, upper_blocks, pair_index(2, 0), t0)],
    )
    t0 = done[0]
    y1 = apply("b1", s1, None)
    v1, _ = gather(y1, [("b01", upper_blocks, pair_index(1, 0))], [])
    target = apply("b01", v1, t0)
    s0, _ = gather(target, [("b0", upper_inv, 0)], [])
    y0 = apply("b0", s0, None)
    v0, _ = gather(y0, [], [])
    wholes = [v0, v1, v2, v3]
    owns = [y0, y1, y2, y3]
    picked = exchange(pick_blocks(ids, wholes, owns), SLICES)
    return leaf_backward(
        leaf_tiles,
        picked.reshape(columns, -1),
        leaf_upper_panel,
        leaf_upper_inv,
        solved,
        levels,
    )


def solution(mesh):
    finer = Mesh(
        mesh.devices.reshape(mesh.shape["gz"], 4, 2, mesh.shape["col"]),
        ("gz", "row_0", "row_1", "col"),
    )
    in_specs = (
        P(GZ_ROW_COL, None, None),
        P(GZ_ROW_COL, None, None),
        P(GZ_ROW_COL, None, None),
        P(GZ_ROW_COL, None, None),
        P(GZ_ROW_COL, None, None),
        P(GZ_ROW_COL),
        P(GZ_ROW_COL, None),
        P(None, ROW_COL, None),
        P(None, ROW_COL, None),
        P(None, ROW_COL, None),
        P(None, ROW_COL, None),
        P(None, ROW_COL, None),
    )
    out_specs = (P(GZ_ROW_COL, None, None), P(None, ROW_COL, None))

    return jax.shard_map(
        body, mesh=finer, in_specs=in_specs, out_specs=out_specs, check_vma=False
    )
```

```python
import jax
import jax.numpy as jnp
from jax import lax
from jax.experimental import pallas as pl
from jax.experimental.pallas import tpu as pltpu
from jax.sharding import Mesh
from jax.sharding import PartitionSpec as P


TILE = 128
ROW_COL = ("row_0", "row_1", "col")
GZ_ROW_COL = ("gz", "row_0", "row_1", "col")
CHIPS = ("row_0", "col")
SLICES = ("gz", "row_1")
SWAP = [(0, 1), (1, 0)]
NT = (((1,), (1,)), ((), ()))
BF16 = jnp.bfloat16
F32 = jnp.float32


def pair_index(higher, lower):
    return higher * (higher - 1) // 2 + lower


def params(mebibytes):
    return pltpu.CompilerParams(vmem_limit_bytes=int(mebibytes * 2**20))


def vmem():
    return pl.BlockSpec(memory_space=pltpu.VMEM)


def smem():
    return pl.BlockSpec(memory_space=pltpu.SMEM)


def anywhere():
    return pl.BlockSpec(memory_space=pl.ANY)


def hbm():
    return pl.BlockSpec(memory_space=pltpu.HBM)


def live_mask(tiles_ref, rows, columns):
    return lax.broadcasted_iota(jnp.int32, (rows, columns), 0) < tiles_ref[0] * TILE


def row_copies(source, target, sems, first, pieces):
    rows = target.shape[0] // pieces
    return [
        pltpu.make_async_copy(
            source.at[pl.ds(k * rows, rows)], target.at[pl.ds(k * rows, rows)], sems.at[first + k]
        )
        for k in range(pieces)
    ]


def leaf_forward(place, tiles, coupled, probe, inverse, panel, top_probe, width):
    rows, columns = probe.shape[1:]
    blocks = coupled.shape[1]
    panel_rows = panel.shape[1]
    levels, top_rows, _ = top_probe.shape

    def kernel(
        place_ref,
        tiles_ref,
        coupled_ref,
        probe_ref,
        inverse_ref,
        panel_ref,
        top_ref,
        out_ref,
        solved_ref,
        mine_ref,
        other_ref,
        pr,
        iv,
        pn,
        tp,
        turned,
        sems,
    ):
        probe_copy = pltpu.make_async_copy(probe_ref.at[0], pr, sems.at[0])
        top_copy = pltpu.make_async_copy(top_ref, tp, sems.at[1])
        inverse_copies = row_copies(inverse_ref.at[0], iv, sems, 2, 4)
        panel_copies = row_copies(panel_ref.at[0], pn, sems, 6, 4)
        for copy in [top_copy, probe_copy] + inverse_copies + panel_copies:
            copy.start()
        live = live_mask(tiles_ref, rows, columns)
        lane = lax.broadcasted_iota(jnp.int32, (columns, TILE), 1)
        ids = jnp.zeros((columns, TILE), F32)
        for j in range(blocks):
            ids = jnp.where(lane == j, coupled_ref[0, j].astype(F32), ids)
        out_ref[:, panel_rows:] = ids.astype(BF16)
        here = place_ref[0]
        there = here + 1 - 2 * lax.rem(here, 2)
        top_copy.wait()
        for level in range(levels):
            turned[level] = tp[level].astype(F32).T
        for index, ref in ((here, mine_ref), (there, other_ref)):
            start = pl.multiple_of(index * width, width)
            for level in range(levels):
                ref[level] = turned[level, pl.ds(start, width), :].astype(BF16)
        probe_copy.wait()
        masked = jnp.where(live, pr[...], jnp.zeros((rows, columns), BF16))
        for copy in inverse_copies:
            copy.wait()
        solved = jnp.dot(iv[...], masked, preferred_element_type=F32)
        solved = jnp.where(live, solved, 0.0)
        solved_ref[...] = solved.astype(BF16)
        across = solved.T.astype(BF16)
        for copy in panel_copies:
            copy.wait()
        out_ref[:, :panel_rows] = lax.dot_general(
            across, pn[...], NT, preferred_element_type=F32
        ).astype(BF16)

    return pl.pallas_call(
        kernel,
        out_shape=(
            jax.ShapeDtypeStruct((columns, panel_rows + TILE), BF16),
            jax.ShapeDtypeStruct((rows, columns), BF16),
            jax.ShapeDtypeStruct((levels, width, top_rows), BF16),
            jax.ShapeDtypeStruct((levels, width, top_rows), BF16),
        ),
        in_specs=[smem(), smem(), smem(), hbm(), hbm(), hbm(), hbm()],
        out_specs=(vmem(), vmem(), vmem(), vmem()),
        scratch_shapes=[
            pltpu.VMEM((rows, columns), BF16),
            pltpu.VMEM((rows, rows), BF16),
            pltpu.VMEM((panel_rows, rows), BF16),
            pltpu.VMEM((levels, top_rows, columns), BF16),
            pltpu.VMEM((levels, columns, top_rows), F32),
            pltpu.SemaphoreType.DMA((10,)),
        ],
        compiler_params=params(63),
        name="leaf_forward",
    )(place, tiles, coupled, probe, inverse, panel, top_probe)


def block_place(block, chip_cols):
    per_chip_row = 2 * chip_cols
    in_level = block % (per_chip_row * (32 // per_chip_row))
    chip = in_level // per_chip_row * chip_cols + in_level % chip_cols
    core = in_level % per_chip_row // chip_cols
    return block // 32, chip, core


def scatter_update(exchanged, levels):
    peers, width, _ = exchanged.shape
    blocks = 8
    data = blocks * TILE

    def kernel(ex_ref, out_ref, ids_ref, dense, ids_s, sem):
        ids_ref[...] = ex_ref[:, 0, data:].astype(F32).astype(jnp.int32)
        copy = pltpu.make_async_copy(ids_ref, ids_s, sem)
        copy.start()
        dense[...] = jnp.zeros(dense.shape, F32)
        copy.wait()
        for p in range(peers):
            for j in range(blocks):
                b = ids_s[p, j]
                dense[b] += ex_ref[p, :, j * TILE : (j + 1) * TILE].astype(F32)
        for b in range(levels * 32):
            level, chip, core = block_place(b, 4)
            out_ref[chip, level, :, core * TILE : (core + 1) * TILE] = dense[b].astype(BF16)

    return pl.pallas_call(
        kernel,
        out_shape=(
            jax.ShapeDtypeStruct((16, levels, width, 2 * TILE), BF16),
            jax.ShapeDtypeStruct((peers, TILE), jnp.int32),
        ),
        in_specs=[vmem()],
        out_specs=(vmem(), vmem()),
        scratch_shapes=[
            pltpu.VMEM((levels * 32, width, TILE), F32),
            pltpu.SMEM((peers, TILE), jnp.int32),
            pltpu.SemaphoreType.DMA,
        ],
        compiler_params=params(4),
        name="scatter_update",
    )(exchanged)


def reduce_update(place, received, mine, other):
    chips, levels, width, rows = received.shape

    def kernel(place_ref, rec_ref, mine_ref, other_ref, first_ref, *rest_refs):
        low_first = lax.rem(place_ref[0], 2) == 0
        for level in range(levels):
            total = rec_ref[0, level].astype(F32)
            for chip in range(1, chips):
                total = total + rec_ref[chip, level].astype(F32)
            own, partner = mine_ref[level].astype(F32), other_ref[level].astype(F32)
            low = jnp.where(low_first, own, partner)
            high = jnp.where(low_first, partner, own)
            target = jnp.concatenate([low, high], 1) - total
            if level == 0:
                first_ref[...] = jnp.broadcast_to(target.astype(BF16)[None], first_ref.shape)
            else:
                rest_refs[level - 1][...] = target

    return pl.pallas_call(
        kernel,
        out_shape=(jax.ShapeDtypeStruct((chips, width, rows), BF16),)
        + (jax.ShapeDtypeStruct((width, rows), F32),) * (levels - 1),
        in_specs=[smem(), vmem(), vmem(), vmem()],
        out_specs=(vmem(),) * levels,
        compiler_params=params(3),
        name="reduce_update",
    )(place, received, mine, other)


def load_rows(after, own, partner, index):
    rows, sep = own.shape[1:]

    def kernel(after_ref, own_ref, partner_ref, out_ref, sems):
        copies = row_copies(own_ref.at[index], out_ref.at[0], sems, 0, 4)
        copies += row_copies(partner_ref.at[index], out_ref.at[1], sems, 4, 4)
        for copy in copies:
            copy.start()
        for copy in copies:
            copy.wait()

    return pl.pallas_call(
        kernel,
        out_shape=jax.ShapeDtypeStruct((2, rows, sep), BF16),
        in_specs=[anywhere(), hbm(), hbm()],
        out_specs=vmem(),
        scratch_shapes=[pltpu.SemaphoreType.DMA((8,))],
        compiler_params=params(50),
        name="load_rows",
    )(after, own, partner)


def load_pair(after, first, first_index, second, second_index):
    rows, sep = first[0].shape[1:]

    def kernel(after_ref, a_ref, b_ref, c_ref, d_ref, one_ref, two_ref, sems):
        copies = []
        for n, (ref, index, out, half) in enumerate(
            (
                (a_ref, first_index, one_ref, 0),
                (b_ref, first_index, one_ref, 1),
                (c_ref, second_index, two_ref, 0),
                (d_ref, second_index, two_ref, 1),
            )
        ):
            copies += row_copies(ref.at[index], out.at[half], sems, 2 * n, 2)
        for copy in copies:
            copy.start()
        for copy in copies:
            copy.wait()

    shape = jax.ShapeDtypeStruct((2, rows, sep), BF16)
    return pl.pallas_call(
        kernel,
        out_shape=(shape, shape),
        in_specs=[anywhere()] + [hbm()] * 4,
        out_specs=(vmem(), vmem()),
        scratch_shapes=[pltpu.SemaphoreType.DMA((8,))],
        compiler_params=params(50),
        name="load_pair",
    )(after, *first, *second)


def products(core_ref, g_ref, first_weights, second_weights):
    parts = []
    for z in range(4):
        for c in range(2):
            for y in range(4):
                parts.append(g_ref[z * 4 + y, :, c * TILE : (c + 1) * TILE])
    whole = jnp.concatenate(parts, 1)
    mine = lax.dot_general(whole, first_weights(), NT, preferred_element_type=F32)
    other = lax.dot_general(whole, second_weights(), NT, preferred_element_type=F32)
    first = lax.rem(core_ref[0], 2) == 0
    return jnp.where(first, mine, other), jnp.where(first, other, mine)


def apply_loaded(core, gathered, weights, base):
    chips, width, rows = gathered.shape

    def kernel(core_ref, g_ref, w_ref, *refs):
        halves = products(core_ref, g_ref, lambda: w_ref[0], lambda: w_ref[1])
        out_ref = refs[-1]
        for k, half in enumerate(halves):
            lanes = slice(k * TILE, (k + 1) * TILE)
            if base is not None:
                base_ref = refs[0]
                start = base_ref[0][:, lanes] if base.ndim == 3 else base_ref[:, lanes]
                half = start.astype(F32) - half
            out_ref[:, :, lanes] = jnp.broadcast_to(half.astype(BF16)[None], (chips, width, TILE))

    operands = [gathered, weights] + ([] if base is None else [base])
    return pl.pallas_call(
        kernel,
        out_shape=pltpu.VMEM((chips, width, rows), BF16),
        in_specs=[smem()] + [vmem()] * len(operands),
        out_specs=vmem(),
        compiler_params=params(4),
        name="apply_loaded",
    )(core, *operands)


def subtract_rows(after, core, gathered, own, partner, index, base):
    _, width, rows = gathered.shape
    sep = own.shape[2]

    def kernel(after_ref, core_ref, g_ref, own_ref, partner_ref, base_ref, out_ref, w, sems):
        copies = [
            row_copies(own_ref.at[index], w.at[0], sems, 0, 4),
            row_copies(partner_ref.at[index], w.at[1], sems, 4, 4),
        ]
        for copy in copies[0] + copies[1]:
            copy.start()

        def arrived(k):
            for copy in copies[k]:
                copy.wait()
            return w[k]

        halves = products(core_ref, g_ref, lambda: arrived(0), lambda: arrived(1))
        for k, half in enumerate(halves):
            lanes = slice(k * TILE, (k + 1) * TILE)
            start = base_ref[0][:, lanes] if base.ndim == 3 else base_ref[:, lanes]
            out_ref[:, lanes] = start.astype(F32) - half

    return pl.pallas_call(
        kernel,
        out_shape=jax.ShapeDtypeStruct((width, rows), F32),
        in_specs=[anywhere(), smem(), vmem(), hbm(), hbm(), vmem()],
        out_specs=vmem(),
        scratch_shapes=[pltpu.VMEM((2, TILE, sep), BF16), pltpu.SemaphoreType.DMA((8,))],
        compiler_params=params(50),
        name="subtract_rows",
    )(after, core, gathered, own, partner, base)


def pick_upper(after, ids, wholes, owns):
    levels = len(wholes) + 1
    _, width, _ = wholes[0].shape
    peers = ids.shape[0]
    blocks = 8

    def kernel(*refs):
        ids_ref = refs[1]
        whole_refs = refs[2 : 1 + levels]
        own_refs = refs[1 + levels : 2 * levels]
        out_ref, every, ids_s, sem = refs[2 * levels :]
        copy = pltpu.make_async_copy(ids_ref, ids_s, sem)
        copy.start()
        every[0] = jnp.zeros((width, TILE), BF16)
        for b in range(32, levels * 32):
            level, chip, core = block_place(b, 4)
            every[b - 31] = whole_refs[level - 1][chip, :, core * TILE : (core + 1) * TILE]
        for p in range(peers):
            core = p % 2
            for level in range(1, levels):
                start = (blocks + level) * TILE
                out_ref[p, :, start : start + TILE] = own_refs[level - 1][
                    0, :, core * TILE : (core + 1) * TILE
                ]
            start = blocks * TILE
            out_ref[p, :, start : start + TILE] = jnp.zeros((width, TILE), BF16)
        copy.wait()
        for p in range(peers):
            for j in range(blocks):
                index = jnp.maximum(ids_s[p, j] - 31, 0)
                out_ref[p, :, j * TILE : (j + 1) * TILE] = every[index]

    return pl.pallas_call(
        kernel,
        out_shape=jax.ShapeDtypeStruct((peers, width, (blocks + levels) * TILE), BF16),
        in_specs=[anywhere()] + [vmem()] * (2 * levels - 1),
        out_specs=vmem(),
        scratch_shapes=[
            pltpu.VMEM((levels * 32 - 31, width, TILE), BF16),
            pltpu.SMEM((peers, TILE), jnp.int32),
            pltpu.SemaphoreType.DMA,
        ],
        compiler_params=params(4),
        name="pick_upper",
    )(after, ids, *wholes, *owns)


def pick_first(ids, picked, whole, own):
    _, width, _ = whole.shape
    peers, _, length = picked.shape
    blocks = 8

    def kernel(ids_ref, picked_ref, whole_ref, own_ref, out_ref, every, ids_s, sem):
        copy = pltpu.make_async_copy(ids_ref, ids_s, sem)
        copy.start()
        for b in range(32):
            _, chip, core = block_place(b, 4)
            every[b] = whole_ref[chip, :, core * TILE : (core + 1) * TILE]
        for p in range(peers):
            core = p % 2
            start = blocks * TILE
            out_ref[p, :, start : start + TILE] = own_ref[0, :, core * TILE : (core + 1) * TILE]
            start += TILE
            out_ref[p, :, start:] = picked_ref[p, :, start:]
        copy.wait()
        for p in range(peers):
            for j in range(blocks):
                lanes = slice(j * TILE, (j + 1) * TILE)
                b = ids_s[p, j]
                tile = every[jnp.minimum(b, 31)]
                out_ref[p, :, lanes] = jnp.where(b < 32, tile, picked_ref[p, :, lanes])

    return pl.pallas_call(
        kernel,
        out_shape=jax.ShapeDtypeStruct((peers, width, length), BF16),
        in_specs=[vmem()] * 4,
        out_specs=vmem(),
        scratch_shapes=[
            pltpu.VMEM((32, width, TILE), BF16),
            pltpu.SMEM((peers, TILE), jnp.int32),
            pltpu.SemaphoreType.DMA,
        ],
        compiler_params=params(4),
        name="pick_first",
    )(ids, picked, whole, own)


def leaf_backward(tiles, picked, panel, inverse, solved, levels):
    rows, columns = solved.shape
    panel_columns = panel.shape[2]

    def kernel(tiles_ref, picked_ref, panel_ref, inverse_ref, solved_ref, leaf_ref, top_ref):
        live = live_mask(tiles_ref, rows, columns)
        product = lax.dot_general(
            panel_ref[0], picked_ref[:, :panel_columns], NT, preferred_element_type=F32
        )
        target = jnp.where(live, solved_ref[...].astype(F32) - product, 0.0).astype(BF16)
        solution = jnp.dot(inverse_ref[0], target, preferred_element_type=F32)
        leaf_ref[0] = jnp.where(live, solution, 0.0)
        for level in range(levels):
            start = panel_columns + level * TILE
            top_ref[level] = picked_ref[:, start : start + TILE].astype(F32).T

    return pl.pallas_call(
        kernel,
        out_shape=(
            jax.ShapeDtypeStruct((1, rows, columns), F32),
            jax.ShapeDtypeStruct((levels, TILE, columns), F32),
        ),
        in_specs=[smem(), vmem(), vmem(), vmem(), vmem()],
        out_specs=(vmem(), vmem()),
        compiler_params=params(5),
        name="leaf_backward",
    )(tiles, picked, panel, inverse, solved)


def exchange(array, axes):
    return lax.all_to_all(array, axes, 0, 0, tiled=True)


def body(
    leaf_probe,
    leaf_lower_inv,
    leaf_upper_inv,
    leaf_lower_panel,
    leaf_upper_panel,
    leaf_tiles,
    coupled,
    top_probe,
    top_lower_inv,
    top_lower_blocks,
    top_upper_inv,
    top_upper_blocks,
):
    levels = top_probe.shape[0]
    columns = leaf_probe.shape[2]
    peers = lax.axis_size(SLICES)
    width = columns // peers
    place = lax.axis_index(SLICES).astype(jnp.int32).reshape(1)

    def swapped(array):
        return lax.ppermute(array, "row_1", SWAP)

    lower_inv_p = swapped(top_lower_inv)
    lower_first = top_lower_blocks[:1]
    lower_first_p = swapped(lower_first)
    lower_blocks_p = swapped(top_lower_blocks)
    sent, solved, probe_mine, probe_other = leaf_forward(
        place,
        leaf_tiles,
        coupled,
        leaf_probe,
        leaf_lower_inv,
        leaf_lower_panel,
        top_probe,
        width,
    )
    probe_other = swapped(probe_other)
    exchanged = exchange(sent.reshape(peers, width, -1), SLICES)
    exchanged, probe_other = lax.optimization_barrier((exchanged, probe_other))
    dense, ids = scatter_update(exchanged, levels)
    received = exchange(dense, CHIPS)
    target, *rest = reduce_update(place, received, probe_mine, probe_other)

    lower_inv = (top_lower_inv, lower_inv_p)
    lower_blocks = (top_lower_blocks, lower_blocks_p)
    upper_inv, upper_blocks = None, None
    ready = {}

    def gather(target, loads, subtractions):
        if len(loads) == 2:
            (one, first, m), (two, second, n) = loads
            ready[one], ready[two] = load_pair(target, first, m, second, n)
        else:
            for name, arrays, index in loads:
                ready[name] = load_rows(target, *arrays, index)
        results = {}
        for higher, whole, arrays, index, base in subtractions:
            results[higher] = subtract_rows(target, place, whole, *arrays, index, base)
        whole = exchange(target, CHIPS)
        fresh = [ready[name] for name, _, _ in loads]
        whole, fresh, results = lax.optimization_barrier((whole, fresh, results))
        for (name, _, _), value in zip(loads, fresh):
            ready[name] = value
        return whole, results

    def apply(name, whole, base):
        return apply_loaded(place, whole, ready[name], base)

    t1, t2, t3 = rest
    r0, _ = gather(target, [("f0", lower_inv, 0)], [])
    x0 = apply("f0", r0, None)
    w0, _ = gather(x0, [("f10", (top_lower_blocks, lower_first_p), 0)], [])
    target = apply("f10", w0, t1)
    upper_in, target = lax.optimization_barrier(((top_upper_inv, top_upper_blocks), target))
    upper_inv = (upper_in[0], swapped(upper_in[0]))
    r1, _ = gather(target, [("f1", lower_inv, 1)], [])
    x1 = apply("f1", r1, None)
    upper_next, x1 = lax.optimization_barrier((upper_in[1], x1))
    upper_blocks = (upper_next, swapped(upper_next))
    w1, done = gather(
        x1,
        [("f21", lower_blocks, pair_index(2, 1))],
        [(2, w0, lower_blocks, pair_index(2, 0), t2)],
    )
    target = apply("f21", w1, done[2])
    r2, done = gather(
        target,
        [("f2", lower_inv, 2)],
        [(3, w0, lower_blocks, pair_index(3, 0), t3)],
    )
    t3 = done[3]
    x2 = apply("f2", r2, None)
    w2, done = gather(
        x2,
        [("f32", lower_blocks, pair_index(3, 2))],
        [(3, w1, lower_blocks, pair_index(3, 1), t3)],
    )
    target = apply("f32", w2, done[3])
    r3, _ = gather(target, [("f3", lower_inv, 3)], [])
    x3 = apply("f3", r3, None)

    s3, _ = gather(x3, [("b3", upper_inv, 3)], [])
    y3 = apply("b3", s3, None)
    v3, _ = gather(y3, [("b23", upper_blocks, pair_index(3, 2))], [])
    target = apply("b23", v3, x2)
    s2, done = gather(
        target,
        [("b2", upper_inv, 2)],
        [(1, v3, upper_blocks, pair_index(3, 1), x1)],
    )
    t1 = done[1]
    y2 = apply("b2", s2, None)
    v2, done = gather(
        y2,
        [("b12", upper_blocks, pair_index(2, 1))],
        [(0, v3, upper_blocks, pair_index(3, 0), x0)],
    )
    t0 = done[0]
    target = apply("b12", v2, t1)
    s1, done = gather(
        target,
        [("b1", upper_inv, 1)],
        [(0, v2, upper_blocks, pair_index(2, 0), t0)],
    )
    t0 = done[0]
    y1 = apply("b1", s1, None)
    v1, _ = gather(y1, [("b01", upper_blocks, pair_index(1, 0))], [])
    target = apply("b01", v1, t0)
    picked = pick_upper(target, ids, [v1, v2, v3], [y1, y2, y3])
    s0, _ = gather(target, [("b0", upper_inv, 0)], [])
    s0, picked = lax.optimization_barrier((s0, picked))
    y0 = apply("b0", s0, None)
    v0, _ = gather(y0, [], [])
    picked = exchange(pick_first(ids, picked, v0, y0), SLICES)
    return leaf_backward(
        leaf_tiles,
        picked.reshape(columns, -1),
        leaf_upper_panel,
        leaf_upper_inv,
        solved,
        levels,
    )


def solution(mesh):
    finer = Mesh(
        mesh.devices.reshape(mesh.shape["gz"], 4, 2, mesh.shape["col"]),
        ("gz", "row_0", "row_1", "col"),
    )
    in_specs = (
        P(GZ_ROW_COL, None, None),
        P(GZ_ROW_COL, None, None),
        P(GZ_ROW_COL, None, None),
        P(GZ_ROW_COL, None, None),
        P(GZ_ROW_COL, None, None),
        P(GZ_ROW_COL),
        P(GZ_ROW_COL, None),
        P(None, ROW_COL, None),
        P(None, ROW_COL, None),
        P(None, ROW_COL, None),
        P(None, ROW_COL, None),
        P(None, ROW_COL, None),
    )
    out_specs = (P(GZ_ROW_COL, None, None), P(None, ROW_COL, None))

    return jax.shard_map(
        body, mesh=finer, in_specs=in_specs, out_specs=out_specs, check_vma=False
    )
```

```python
import jax
import jax.numpy as jnp
from jax import lax
from jax.experimental import pallas as pl
from jax.experimental.pallas import tpu as pltpu
from jax.sharding import Mesh
from jax.sharding import PartitionSpec as P


TILE = 128
ROW_COL = ("row_0", "row_1", "col")
GZ_ROW_COL = ("gz", "row_0", "row_1", "col")
CHIPS = ("row_0", "col")
SLICES = ("gz", "row_1")
SWAP = [(0, 1), (1, 0)]
NT = (((1,), (1,)), ((), ()))
BF16 = jnp.bfloat16
F32 = jnp.float32


def pair_index(higher, lower):
    return higher * (higher - 1) // 2 + lower


def params(mebibytes):
    return pltpu.CompilerParams(vmem_limit_bytes=int(mebibytes * 2**20))


def vmem():
    return pl.BlockSpec(memory_space=pltpu.VMEM)


def smem():
    return pl.BlockSpec(memory_space=pltpu.SMEM)


def anywhere():
    return pl.BlockSpec(memory_space=pl.ANY)


def hbm():
    return pl.BlockSpec(memory_space=pltpu.HBM)


def live_mask(tiles_ref, rows, columns):
    return lax.broadcasted_iota(jnp.int32, (rows, columns), 0) < tiles_ref[0] * TILE


def row_copies(source, target, sems, first, pieces):
    rows = target.shape[0] // pieces
    return [
        pltpu.make_async_copy(
            source.at[pl.ds(k * rows, rows)], target.at[pl.ds(k * rows, rows)], sems.at[first + k]
        )
        for k in range(pieces)
    ]


def leaf_forward(place, tiles, coupled, probe, inverse, panel, top_probe, lower, width):
    rows, columns = probe.shape[1:]
    blocks = coupled.shape[1]
    panel_rows = panel.shape[1]
    levels, top_rows, _ = top_probe.shape

    def kernel(
        place_ref,
        tiles_ref,
        coupled_ref,
        probe_ref,
        inverse_ref,
        panel_ref,
        top_ref,
        lower_ref,
        out_ref,
        solved_ref,
        mine_ref,
        other_ref,
        first_ref,
        pr,
        iv,
        pn,
        tp,
        turned,
        first,
        sems,
    ):
        probe_copy = pltpu.make_async_copy(probe_ref.at[0], pr, sems.at[0])
        top_copy = pltpu.make_async_copy(top_ref, tp, sems.at[1])
        inverse_copies = row_copies(inverse_ref.at[0], iv, sems, 2, 4)
        panel_copies = row_copies(panel_ref.at[0], pn, sems, 6, 4)
        first_copies = row_copies(lower_ref.at[0], first, sems, 10, 4)
        out_copies = row_copies(first, first_ref.at[0], sems, 14, 4)
        for copy in [top_copy, probe_copy] + inverse_copies + panel_copies + first_copies:
            copy.start()
        live = live_mask(tiles_ref, rows, columns)
        lane = lax.broadcasted_iota(jnp.int32, (columns, TILE), 1)
        ids = jnp.zeros((columns, TILE), F32)
        for j in range(blocks):
            ids = jnp.where(lane == j, coupled_ref[0, j].astype(F32), ids)
        out_ref[:, panel_rows:] = ids.astype(BF16)
        here = place_ref[0]
        there = here + 1 - 2 * lax.rem(here, 2)
        top_copy.wait()
        for level in range(levels):
            turned[level] = tp[level].astype(F32).T
        for index, ref in ((here, mine_ref), (there, other_ref)):
            start = pl.multiple_of(index * width, width)
            for level in range(levels):
                ref[level] = turned[level, pl.ds(start, width), :].astype(BF16)
        probe_copy.wait()
        masked = jnp.where(live, pr[...], jnp.zeros((rows, columns), BF16))
        for copy in inverse_copies:
            copy.wait()
        solved = jnp.dot(iv[...], masked, preferred_element_type=F32)
        solved = jnp.where(live, solved, 0.0)
        solved_ref[...] = solved.astype(BF16)
        across = solved.T.astype(BF16)
        for copy in first_copies:
            copy.wait()
        for copy in out_copies:
            copy.start()
        for copy in panel_copies:
            copy.wait()
        out_ref[:, :panel_rows] = lax.dot_general(
            across, pn[...], NT, preferred_element_type=F32
        ).astype(BF16)
        for copy in out_copies:
            copy.wait()

    return pl.pallas_call(
        kernel,
        out_shape=(
            jax.ShapeDtypeStruct((columns, panel_rows + TILE), BF16),
            jax.ShapeDtypeStruct((rows, columns), BF16),
            jax.ShapeDtypeStruct((levels, width, top_rows), BF16),
            jax.ShapeDtypeStruct((levels, width, top_rows), BF16),
            jax.ShapeDtypeStruct((1, *lower.shape[1:]), BF16),
        ),
        in_specs=[smem(), smem(), smem(), hbm(), hbm(), hbm(), hbm(), hbm()],
        out_specs=(vmem(), vmem(), vmem(), vmem(), hbm()),
        scratch_shapes=[
            pltpu.VMEM((rows, columns), BF16),
            pltpu.VMEM((rows, rows), BF16),
            pltpu.VMEM((panel_rows, rows), BF16),
            pltpu.VMEM((levels, top_rows, columns), BF16),
            pltpu.VMEM((levels, columns, top_rows), F32),
            pltpu.VMEM(lower.shape[1:], BF16),
            pltpu.SemaphoreType.DMA((18,)),
        ],
        compiler_params=params(63),
        name="leaf_forward",
    )(place, tiles, coupled, probe, inverse, panel, top_probe, lower)


def block_place(block, chip_cols):
    per_chip_row = 2 * chip_cols
    in_level = block % (per_chip_row * (32 // per_chip_row))
    chip = in_level // per_chip_row * chip_cols + in_level % chip_cols
    core = in_level % per_chip_row // chip_cols
    return block // 32, chip, core


def scatter_update(exchanged, levels):
    peers, width, _ = exchanged.shape
    blocks = 8
    data = blocks * TILE

    def kernel(ex_ref, out_ref, ids_ref, dense, ids_s, sem):
        ids_ref[...] = ex_ref[:, 0, data:].astype(F32).astype(jnp.int32)
        copy = pltpu.make_async_copy(ids_ref, ids_s, sem)
        copy.start()
        dense[...] = jnp.zeros(dense.shape, F32)
        copy.wait()
        for p in range(peers):
            for j in range(blocks):
                b = ids_s[p, j]
                dense[b] += ex_ref[p, :, j * TILE : (j + 1) * TILE].astype(F32)
        for b in range(levels * 32):
            level, chip, core = block_place(b, 4)
            out_ref[chip, level, :, core * TILE : (core + 1) * TILE] = dense[b].astype(BF16)

    return pl.pallas_call(
        kernel,
        out_shape=(
            jax.ShapeDtypeStruct((16, levels, width, 2 * TILE), BF16),
            jax.ShapeDtypeStruct((peers, TILE), jnp.int32),
        ),
        in_specs=[vmem()],
        out_specs=(vmem(), vmem()),
        scratch_shapes=[
            pltpu.VMEM((levels * 32, width, TILE), F32),
            pltpu.SMEM((peers, TILE), jnp.int32),
            pltpu.SemaphoreType.DMA,
        ],
        compiler_params=params(4),
        name="scatter_update",
    )(exchanged)


def reduce_update(place, received, mine, other):
    chips, levels, width, rows = received.shape

    def kernel(place_ref, rec_ref, mine_hbm, other_ref, first_ref, *refs):
        rest_refs = refs[: levels - 1]
        mine_ref, sem = refs[levels - 1 :]
        copy = pltpu.make_async_copy(mine_hbm, mine_ref, sem)
        copy.start()
        low_first = lax.rem(place_ref[0], 2) == 0
        for level in range(levels - 1, -1, -1):
            total = rec_ref[0, level].astype(F32)
            for chip in range(1, chips):
                total = total + rec_ref[chip, level].astype(F32)
            if level == levels - 1:
                copy.wait()
            own, partner = mine_ref[level].astype(F32), other_ref[level].astype(F32)
            low = jnp.where(low_first, own, partner)
            high = jnp.where(low_first, partner, own)
            target = jnp.concatenate([low, high], 1) - total
            if level == 0:
                first_ref[...] = jnp.broadcast_to(target.astype(BF16)[None], first_ref.shape)
            else:
                rest_refs[level - 1][...] = target

    return pl.pallas_call(
        kernel,
        out_shape=(jax.ShapeDtypeStruct((chips, width, rows), BF16),)
        + (jax.ShapeDtypeStruct((width, rows), F32),) * (levels - 1),
        in_specs=[smem(), vmem(), hbm(), vmem()],
        out_specs=(vmem(),) * levels,
        scratch_shapes=[pltpu.VMEM(mine.shape, BF16), pltpu.SemaphoreType.DMA],
        compiler_params=params(3),
        name="reduce_update",
    )(place, received, mine, other)


def load_rows(after, own, partner, index):
    rows, sep = own.shape[1:]

    def kernel(after_ref, own_ref, partner_ref, out_ref, sems):
        copies = row_copies(own_ref.at[index], out_ref.at[0], sems, 0, 4)
        copies += row_copies(partner_ref.at[index], out_ref.at[1], sems, 4, 4)
        for copy in copies:
            copy.start()
        for copy in copies:
            copy.wait()

    return pl.pallas_call(
        kernel,
        out_shape=jax.ShapeDtypeStruct((2, rows, sep), BF16),
        in_specs=[anywhere(), hbm(), hbm()],
        out_specs=vmem(),
        scratch_shapes=[pltpu.SemaphoreType.DMA((8,))],
        compiler_params=params(50),
        name="load_rows",
    )(after, own, partner)


def load_pair(after, first, first_index, second, second_index):
    rows, sep = first[0].shape[1:]

    def kernel(after_ref, a_ref, b_ref, c_ref, d_ref, one_ref, two_ref, sems):
        copies = []
        for n, (ref, index, out, half) in enumerate(
            (
                (a_ref, first_index, one_ref, 0),
                (b_ref, first_index, one_ref, 1),
                (c_ref, second_index, two_ref, 0),
                (d_ref, second_index, two_ref, 1),
            )
        ):
            copies += row_copies(ref.at[index], out.at[half], sems, 2 * n, 2)
        for copy in copies:
            copy.start()
        for copy in copies:
            copy.wait()

    shape = jax.ShapeDtypeStruct((2, rows, sep), BF16)
    return pl.pallas_call(
        kernel,
        out_shape=(shape, shape),
        in_specs=[anywhere()] + [hbm()] * 4,
        out_specs=(vmem(), vmem()),
        scratch_shapes=[pltpu.SemaphoreType.DMA((8,))],
        compiler_params=params(50),
        name="load_pair",
    )(after, *first, *second)


def products(core_ref, g_ref, first_weights, second_weights):
    parts = []
    for z in range(4):
        for c in range(2):
            for y in range(4):
                parts.append(g_ref[z * 4 + y, :, c * TILE : (c + 1) * TILE])
    whole = jnp.concatenate(parts, 1)
    mine = lax.dot_general(whole, first_weights(), NT, preferred_element_type=F32)
    other = lax.dot_general(whole, second_weights(), NT, preferred_element_type=F32)
    first = lax.rem(core_ref[0], 2) == 0
    return jnp.where(first, mine, other), jnp.where(first, other, mine)


def apply_loaded(core, gathered, weights, base):
    chips, width, rows = gathered.shape

    def kernel(core_ref, g_ref, w_ref, *refs):
        halves = products(core_ref, g_ref, lambda: w_ref[0], lambda: w_ref[1])
        out_ref, small_ref = refs[-2:]
        for k, half in enumerate(halves):
            lanes = slice(k * TILE, (k + 1) * TILE)
            if base is not None:
                base_ref = refs[0]
                half = base_ref[:, lanes].astype(F32) - half
            half = half.astype(BF16)
            small_ref[:, lanes] = half
            out_ref[:, :, lanes] = jnp.broadcast_to(half[None], (chips, width, TILE))

    operands = [gathered, weights] + ([] if base is None else [base])
    return pl.pallas_call(
        kernel,
        out_shape=(
            jax.ShapeDtypeStruct((chips, width, rows), BF16),
            jax.ShapeDtypeStruct((width, rows), BF16),
        ),
        in_specs=[smem()] + [vmem()] * len(operands),
        out_specs=(vmem(), vmem()),
        compiler_params=params(4),
        name="apply_loaded",
    )(core, *operands)


def subtract_rows(after, core, gathered, own, partner, index, base):
    _, width, rows = gathered.shape
    sep = own.shape[2]

    def kernel(after_ref, core_ref, g_ref, own_ref, partner_ref, base_ref, out_ref, w, sems):
        copies = [
            row_copies(own_ref.at[index], w.at[0], sems, 0, 4),
            row_copies(partner_ref.at[index], w.at[1], sems, 4, 4),
        ]
        for copy in copies[0] + copies[1]:
            copy.start()

        def arrived(k):
            for copy in copies[k]:
                copy.wait()
            return w[k]

        halves = products(core_ref, g_ref, lambda: arrived(0), lambda: arrived(1))
        for k, half in enumerate(halves):
            lanes = slice(k * TILE, (k + 1) * TILE)
            out_ref[:, lanes] = base_ref[:, lanes].astype(F32) - half

    return pl.pallas_call(
        kernel,
        out_shape=jax.ShapeDtypeStruct((width, rows), F32),
        in_specs=[anywhere(), smem(), vmem(), hbm(), hbm(), vmem()],
        out_specs=vmem(),
        scratch_shapes=[pltpu.VMEM((2, TILE, sep), BF16), pltpu.SemaphoreType.DMA((8,))],
        compiler_params=params(50),
        name="subtract_rows",
    )(after, core, gathered, own, partner, base)


def pick_upper(after, ids, wholes, owns):
    levels = len(wholes) + 1
    _, width, _ = wholes[0].shape
    peers = ids.shape[0]
    blocks = 8

    def kernel(*refs):
        ids_ref = refs[1]
        whole_refs = refs[2 : 1 + levels]
        own_refs = refs[1 + levels : 2 * levels]
        out_ref, every, ids_s, sem = refs[2 * levels :]
        copy = pltpu.make_async_copy(ids_ref, ids_s, sem)
        copy.start()
        every[0] = jnp.zeros((width, TILE), BF16)
        for b in range(32, levels * 32):
            level, chip, core = block_place(b, 4)
            every[b - 31] = whole_refs[level - 1][chip, :, core * TILE : (core + 1) * TILE]
        for p in range(peers):
            core = p % 2
            for level in range(1, levels):
                start = (blocks + level) * TILE
                out_ref[p, :, start : start + TILE] = own_refs[level - 1][
                    :, core * TILE : (core + 1) * TILE
                ]
            start = blocks * TILE
            out_ref[p, :, start : start + TILE] = jnp.zeros((width, TILE), BF16)
        copy.wait()
        for p in range(peers):
            for j in range(blocks):
                index = jnp.maximum(ids_s[p, j] - 31, 0)
                out_ref[p, :, j * TILE : (j + 1) * TILE] = every[index]

    return pl.pallas_call(
        kernel,
        out_shape=jax.ShapeDtypeStruct((peers, width, (blocks + levels) * TILE), BF16),
        in_specs=[anywhere()] + [vmem()] * (2 * levels - 1),
        out_specs=vmem(),
        scratch_shapes=[
            pltpu.VMEM((levels * 32 - 31, width, TILE), BF16),
            pltpu.SMEM((peers, TILE), jnp.int32),
            pltpu.SemaphoreType.DMA,
        ],
        compiler_params=params(4),
        name="pick_upper",
    )(after, ids, *wholes, *owns)


def pick_first(ids, picked, whole, own):
    _, width, _ = whole.shape
    peers, _, length = picked.shape
    blocks = 8

    def kernel(ids_ref, picked_ref, whole_ref, own_ref, out_ref, every, ids_s, sem):
        copy = pltpu.make_async_copy(ids_ref, ids_s, sem)
        copy.start()
        for b in range(32):
            _, chip, core = block_place(b, 4)
            every[b] = whole_ref[chip, :, core * TILE : (core + 1) * TILE]
        for p in range(peers):
            core = p % 2
            start = blocks * TILE
            out_ref[p, :, start : start + TILE] = own_ref[:, core * TILE : (core + 1) * TILE]
            start += TILE
            out_ref[p, :, start:] = picked_ref[p, :, start:]
        copy.wait()
        for p in range(peers):
            for j in range(blocks):
                lanes = slice(j * TILE, (j + 1) * TILE)
                b = ids_s[p, j]
                tile = every[jnp.minimum(b, 31)]
                out_ref[p, :, lanes] = jnp.where(b < 32, tile, picked_ref[p, :, lanes])

    return pl.pallas_call(
        kernel,
        out_shape=jax.ShapeDtypeStruct((peers, width, length), BF16),
        in_specs=[vmem()] * 4,
        out_specs=vmem(),
        scratch_shapes=[
            pltpu.VMEM((32, width, TILE), BF16),
            pltpu.SMEM((peers, TILE), jnp.int32),
            pltpu.SemaphoreType.DMA,
        ],
        compiler_params=params(4),
        name="pick_first",
    )(ids, picked, whole, own)


def leaf_backward(tiles, picked, panel, inverse, solved, levels):
    rows, columns = solved.shape
    panel_columns = panel.shape[2]

    def kernel(tiles_ref, picked_ref, panel_ref, inverse_ref, solved_ref, leaf_ref, top_ref):
        live = live_mask(tiles_ref, rows, columns)
        product = lax.dot_general(
            panel_ref[0], picked_ref[:, :panel_columns], NT, preferred_element_type=F32
        )
        target = jnp.where(live, solved_ref[...].astype(F32) - product, 0.0).astype(BF16)
        solution = jnp.dot(inverse_ref[0], target, preferred_element_type=F32)
        leaf_ref[0] = jnp.where(live, solution, 0.0)
        for level in range(levels):
            start = panel_columns + level * TILE
            top_ref[level] = picked_ref[:, start : start + TILE].astype(F32).T

    return pl.pallas_call(
        kernel,
        out_shape=(
            jax.ShapeDtypeStruct((1, rows, columns), F32),
            jax.ShapeDtypeStruct((levels, TILE, columns), F32),
        ),
        in_specs=[smem(), vmem(), vmem(), vmem(), vmem()],
        out_specs=(vmem(), vmem()),
        compiler_params=params(5),
        name="leaf_backward",
    )(tiles, picked, panel, inverse, solved)


def exchange(array, axes):
    return lax.all_to_all(array, axes, 0, 0, tiled=True)


def body(
    leaf_probe,
    leaf_lower_inv,
    leaf_upper_inv,
    leaf_lower_panel,
    leaf_upper_panel,
    leaf_tiles,
    coupled,
    top_probe,
    top_lower_inv,
    top_lower_blocks,
    top_upper_inv,
    top_upper_blocks,
):
    levels = top_probe.shape[0]
    columns = leaf_probe.shape[2]
    peers = lax.axis_size(SLICES)
    width = columns // peers
    place = lax.axis_index(SLICES).astype(jnp.int32).reshape(1)

    def swapped(array):
        return lax.ppermute(array, "row_1", SWAP)

    lower_inv_p = swapped(top_lower_inv)
    lower_blocks_p = swapped(top_lower_blocks)
    sent, solved, probe_mine, probe_other, lower_first = leaf_forward(
        place,
        leaf_tiles,
        coupled,
        leaf_probe,
        leaf_lower_inv,
        leaf_lower_panel,
        top_probe,
        top_lower_blocks,
        width,
    )
    probe_other = swapped(probe_other)
    lower_first_p = swapped(lower_first)
    exchanged = exchange(sent.reshape(peers, width, -1), SLICES)
    dense, ids = scatter_update(exchanged, levels)
    received = exchange(dense, CHIPS)
    target, *rest = reduce_update(place, received, probe_mine, probe_other)

    lower_inv = (top_lower_inv, lower_inv_p)
    lower_blocks = (top_lower_blocks, lower_blocks_p)
    upper_inv, upper_blocks = None, None
    ready = {}

    def gather(target, loads, subtractions):
        if len(loads) == 2:
            (one, first, m), (two, second, n) = loads
            ready[one], ready[two] = load_pair(target, first, m, second, n)
        else:
            for name, arrays, index in loads:
                ready[name] = load_rows(target, *arrays, index)
        results = {}
        for higher, whole, arrays, index, base in subtractions:
            results[higher] = subtract_rows(target, place, whole, *arrays, index, base)
        whole = exchange(target, CHIPS)
        fresh = [ready[name] for name, _, _ in loads]
        whole, fresh, results = lax.optimization_barrier((whole, fresh, results))
        for (name, _, _), value in zip(loads, fresh):
            ready[name] = value
        return whole, results

    def apply(name, whole, base):
        return apply_loaded(place, whole, ready[name], base)

    t1, t2, t3 = rest
    r0, _ = gather(target, [("f0", lower_inv, 0)], [])
    x0, x0_own = apply("f0", r0, None)
    w0, _ = gather(x0, [("f10", (top_lower_blocks, lower_first_p), 0)], [])
    target, _ = apply("f10", w0, t1)
    upper_in, target = lax.optimization_barrier(((top_upper_inv, top_upper_blocks), target))
    upper_inv = (upper_in[0], swapped(upper_in[0]))
    r1, _ = gather(target, [("f1", lower_inv, 1)], [])
    x1, x1_own = apply("f1", r1, None)
    upper_next, x1 = lax.optimization_barrier((upper_in[1], x1))
    upper_blocks = (upper_next, swapped(upper_next))
    w1, done = gather(
        x1,
        [("f21", lower_blocks, pair_index(2, 1))],
        [(2, w0, lower_blocks, pair_index(2, 0), t2)],
    )
    target, _ = apply("f21", w1, done[2])
    r2, done = gather(
        target,
        [("f2", lower_inv, 2)],
        [(3, w0, lower_blocks, pair_index(3, 0), t3)],
    )
    t3 = done[3]
    x2, x2_own = apply("f2", r2, None)
    w2, done = gather(
        x2,
        [("f32", lower_blocks, pair_index(3, 2))],
        [(3, w1, lower_blocks, pair_index(3, 1), t3)],
    )
    target, _ = apply("f32", w2, done[3])
    r3, _ = gather(target, [("f3", lower_inv, 3)], [])
    x3, _ = apply("f3", r3, None)

    s3, _ = gather(x3, [("b3", upper_inv, 3)], [])
    y3, y3_own = apply("b3", s3, None)
    v3, _ = gather(y3, [("b23", upper_blocks, pair_index(3, 2))], [])
    target, _ = apply("b23", v3, x2_own)
    s2, done = gather(
        target,
        [("b2", upper_inv, 2)],
        [(1, v3, upper_blocks, pair_index(3, 1), x1_own)],
    )
    t1 = done[1]
    y2, y2_own = apply("b2", s2, None)
    v2, done = gather(
        y2,
        [("b12", upper_blocks, pair_index(2, 1))],
        [(0, v3, upper_blocks, pair_index(3, 0), x0_own)],
    )
    t0 = done[0]
    target, _ = apply("b12", v2, t1)
    s1, done = gather(
        target,
        [("b1", upper_inv, 1)],
        [(0, v2, upper_blocks, pair_index(2, 0), t0)],
    )
    t0 = done[0]
    y1, y1_own = apply("b1", s1, None)
    v1, _ = gather(y1, [("b01", upper_blocks, pair_index(1, 0))], [])
    target, _ = apply("b01", v1, t0)
    picked = pick_upper(target, ids, [v1, v2, v3], [y1_own, y2_own, y3_own])
    s0, _ = gather(target, [("b0", upper_inv, 0)], [])
    s0, picked = lax.optimization_barrier((s0, picked))
    y0, y0_own = apply("b0", s0, None)
    v0, _ = gather(y0, [], [])
    picked = exchange(pick_first(ids, picked, v0, y0_own), SLICES)
    return leaf_backward(
        leaf_tiles,
        picked.reshape(columns, -1),
        leaf_upper_panel,
        leaf_upper_inv,
        solved,
        levels,
    )


def solution(mesh):
    finer = Mesh(
        mesh.devices.reshape(mesh.shape["gz"], 4, 2, mesh.shape["col"]),
        ("gz", "row_0", "row_1", "col"),
    )
    in_specs = (
        P(GZ_ROW_COL, None, None),
        P(GZ_ROW_COL, None, None),
        P(GZ_ROW_COL, None, None),
        P(GZ_ROW_COL, None, None),
        P(GZ_ROW_COL, None, None),
        P(GZ_ROW_COL),
        P(GZ_ROW_COL, None),
        P(None, ROW_COL, None),
        P(None, ROW_COL, None),
        P(None, ROW_COL, None),
        P(None, ROW_COL, None),
        P(None, ROW_COL, None),
    )
    out_specs = (P(GZ_ROW_COL, None, None), P(None, ROW_COL, None))

    return jax.shard_map(
        body, mesh=finer, in_specs=in_specs, out_specs=out_specs, check_vma=False
    )
```
